32 devices in a mesh: tube: 4 (over z), col: 2 (over y), row: 4 (over x, core).
Axes of the slice: x: 2, y: 2, z: 4, core: 2. Of those that a mesh axis runs over, the one named last changes fastest.
Arguments:
- tensor: float32 [16, 2048, 8192], P('tube', 'row', 'col')
- b_init: float32 [8192, 256], P(('col', 'row', 'tube'))
- c_init: float32 [16, 256], replicated
- ridge_lam: float32 [], replicated
Outputs:
- output 1: float32 [2048, 256], P(('row', 'col', 'tube'))
- output 2: float32 [8192, 256], P(('col', 'row', 'tube'))
- output 3: float32 [16, 256], replicated
All inputs are finite; a program needn't handle non-finite values.
Results may differ from the reference program's by a relative error of at most 0.00544.
Values are sent between devices in bfloat16 or wider.
A program may use at most 1 GiB of HBM per device.

```python
import jax
import jax.numpy as jnp
from jax import lax

K_LEN = 16
CP_RANK = 256
I_ROWS = 2048
J_ROWS = 8192
SWEEPS = 2


def setup_inputs(seed: int = 0) -> dict:
    keys = jax.random.split(jax.random.key(seed), 7)
    scale = CP_RANK ** (-1.0 / 6.0)
    fac_a = scale * jax.random.normal(keys[0], (I_ROWS, CP_RANK), jnp.float32)
    fac_b = scale * jax.random.normal(keys[1], (J_ROWS, CP_RANK), jnp.float32)
    fac_c = scale * jax.random.normal(keys[2], (K_LEN, CP_RANK), jnp.float32)
    kir_prod = fac_c[:, None, :] * fac_a[None, :, :]
    planted = jnp.einsum("kir,jr->kij", kir_prod, fac_b)
    noise = 0.3 * jax.random.normal(keys[3], (K_LEN, I_ROWS, J_ROWS), jnp.float32)
    b_init = fac_b + scale * jax.random.normal(keys[4], (J_ROWS, CP_RANK), jnp.float32)
    c_init = fac_c + scale * jax.random.normal(keys[5], (K_LEN, CP_RANK), jnp.float32)
    ridge_lam = jax.random.uniform(keys[6], (), jnp.float32, 0.1, 0.3) * (J_ROWS * K_LEN * CP_RANK ** (-2.0 / 3.0))
    return {"tensor": planted + noise, "b_init": b_init, "c_init": c_init, "ridge_lam": ridge_lam}


def gram_of(factor):
    half_fac = factor.astype(jnp.bfloat16)
    return jnp.dot(half_fac.T, half_fac, preferred_element_type=jnp.float32)


def solve_rows(mttkrp_rows, gram_prod, ridge_lam):
    ident_mat = jnp.eye(gram_prod.shape[0], dtype=gram_prod.dtype)
    chol_fac = jnp.linalg.cholesky(gram_prod + ridge_lam * ident_mat)
    half_solve = lax.linalg.triangular_solve(chol_fac, mttkrp_rows, left_side=False, lower=True, transpose_a=True)
    return lax.linalg.triangular_solve(chol_fac, half_solve, left_side=False, lower=True)


def reference(tensor, b_init, c_init, ridge_lam):
    x_half = tensor.astype(jnp.bfloat16)
    flat_x = x_half.reshape(K_LEN * I_ROWS, J_ROWS)
    fac_b = b_init
    fac_c = c_init
    gram_b = gram_of(fac_b)
    for sweep_idx in range(SWEEPS):
        gram_c = gram_of(fac_c)
        u_kir = jnp.dot(flat_x, fac_b.astype(jnp.bfloat16), preferred_element_type=jnp.float32).reshape(K_LEN, I_ROWS, CP_RANK)
        mtt_a = jnp.einsum("kir,kr->ir", u_kir.astype(jnp.float32), fac_c.astype(jnp.float32))
        fac_a = solve_rows(mtt_a, gram_b * gram_c, ridge_lam)
        gram_a = gram_of(fac_a)
        a_half = fac_a.astype(jnp.bfloat16)
        v_kjr = lax.map(lambda slab: lax.dot_general(slab, a_half, (((0,), (0,)), ((), ())), preferred_element_type=jnp.float32), x_half)
        mtt_b = jnp.einsum("kjr,kr->jr", v_kjr.astype(jnp.float32), fac_c.astype(jnp.float32))
        fac_b = solve_rows(mtt_b, gram_a * gram_c, ridge_lam)
        gram_b = gram_of(fac_b)
        u_kir = jnp.dot(flat_x, fac_b.astype(jnp.bfloat16), preferred_element_type=jnp.float32).reshape(K_LEN, I_ROWS, CP_RANK)
        mtt_c = jnp.einsum("kir,ir->kr", u_kir.astype(jnp.float32), fac_a.astype(jnp.float32))
        fac_c = solve_rows(mtt_c, gram_a * gram_b, ridge_lam)
    return fac_a, fac_b, fac_c
```

```python
import jax
import jax.numpy as jnp
from jax import lax
from jax.experimental import pallas as pl
from jax.experimental.pallas import tpu as pltpu
from jax.sharding import PartitionSpec as P

SWEEPS = 2
F32 = jnp.float32
BF16 = jnp.bfloat16
HI = lax.Precision.HIGHEST
MESH = pl.DeviceIdType.MESH
RANK = 256
PIV = 16
ROWS_T = 64
STAGES = 4


def dot32(lhs, rhs, lhs_dim, rhs_dim):
    return lax.dot_general(lhs, rhs, (((lhs_dim,), (rhs_dim,)), ((), ())), precision=HI, preferred_element_type=F32)


def dot16(lhs, rhs, lhs_dim, rhs_dim):
    return lax.dot_general(lhs, rhs, (((lhs_dim,), (rhs_dim,)), ((), ())), preferred_element_type=F32)


def factor_block(blk, w_ref, inv_ref, idx):
    size = 128
    lane = lax.broadcasted_iota(jnp.int32, (PIV, size), 1)
    row = lax.broadcasted_iota(jnp.int32, (PIV, size), 0)
    lanes = lax.broadcasted_iota(jnp.int32, (size, size), 1)
    lo = pl.multiple_of(blk * PIV, PIV)
    slab = w_ref[pl.ds(lo, PIV)]
    full = w_ref[...]
    cols = jnp.stack([jnp.broadcast_to(slab[:, q:q + 1], (PIV, size)) for q in range(PIV)])
    work = pltpu.roll(jnp.where(lane < PIV, jnp.where(lane == row, 1.0, 0.0), slab), size - PIV, 1)
    rest = pltpu.roll(jnp.where(lanes < PIV, 0.0, full), size - PIV, 1)
    scale = jnp.ones((PIV, size), F32)
    low = work
    for q in range(PIV):
        here = row == q
        piv = cols[0, q:q + 1]
        rec = 1.0 / piv
        mult = jnp.where(here, 0.0, cols[0] * rec)
        low = jnp.where(here, work * lax.rsqrt(piv), low)
        scale = jnp.where(here, rec, scale)
        work = work - mult * work[q:q + 1]
        if q + 1 < PIV:
            cols = cols[1:] - mult[None] * cols[1:, q:q + 1]
    mid = work * scale
    for q in range(PIV):
        rest = rest - full[:, q:q + 1] * mid[q:q + 1]
    w_ref[...] = rest
    low = jnp.where(lane >= size - PIV - lo, low, 0.0)
    inv_ref[idx, pl.ds(lo, PIV)] = pltpu.roll(low, lo + PIV, 1)


def inv_chol(mat, w_ref, inv_ref, low_ref):
    below = mat[128:, :128]
    corner = mat[128:, 128:]
    w_ref[...] = mat[:128, :128]

    def step(idx, carry):
        lax.fori_loop(0, 128 // PIV, lambda blk, c: (factor_block(blk, w_ref, inv_ref, idx), c)[1], 0)
        low = dot32(below, inv_ref[idx], 1, 1)
        low_ref[idx] = low
        w_ref[...] = corner - dot32(low, low, 1, 1)
        return carry

    lax.fori_loop(0, 2, step, 0)
    first, second = inv_ref[0], inv_ref[1]
    off = -dot32(dot32(second, low_ref[0], 1, 0), first, 1, 0)
    top = jnp.concatenate([first, jnp.zeros((128, 128), F32)], axis=1)
    return jnp.concatenate([top, jnp.concatenate([off, second], axis=1)], axis=0)


def kernel(x_ref, b_ref, c_ref, lam_ref, a_out, b_out, c_out,
           xh, xin, u_buf, pa, pb, ball, a16, a32, ya, za, yb, xb, zb,
           gown, gcore, gpeer, gfin, cmid, cpart, ctot, csplat, at_buf, work, hinv, hlow, linv, gmat_a, gmat_b, c_cur,
           load_sem, s_ab, r_ab, s_a16, r_a16, s_a32, r_a32, s_ya, r_ya, s_za, r_za,
           s_yb, r_yb, s_xb, r_xb, s_zb, r_zb, s_g, r_g, s_c, r_c):
    tube = lax.axis_index("tube")
    col = lax.axis_index("col")
    row = lax.axis_index("row")
    core = lax.rem(row, 2)
    xpos = row // 2
    xrow = lax.rem(row + 2, 4)
    crow = row + 1 - 2 * core
    lam = lam_ref[...]

    def dev(t, c, r):
        return {"tube": t, "col": c, "row": r}

    def shift(d):
        return lax.rem(tube + d, 4)

    peer_x, peer_core, peer_y = dev(tube, col, xrow), dev(tube, col, crow), dev(tube, 1 - col, row)

    def peer_z(d):
        return dev(shift(d), col, row)

    def plane(n):
        other = lax.rem(col * 4 + row + n, 8)
        return dev(tube, other // 4, lax.rem(other, 4))

    barrier = pltpu.get_barrier_semaphore()
    for d in range(1, 4):
        pl.semaphore_signal(barrier, inc=1, device_id=peer_z(d), device_id_type=MESH)
    for n in range(1, 8):
        pl.semaphore_signal(barrier, inc=1, device_id=plane(n), device_id_type=MESH)
    pl.semaphore_wait(barrier, 10)

    def remote(src, dst, send, recv, device):
        return pltpu.make_async_remote_copy(src_ref=src, dst_ref=dst, send_sem=send, recv_sem=recv,
                                            device_id=device, device_id_type=MESH)

    def slot_b(r, t):
        return r * 4 + t

    def ab_copy(v, slot, send, device):
        return remote(ball.at[v, slot], ball.at[v, slot], s_ab.at[v, send], r_ab.at[v, slot], device)

    def ab_start(v):
        own = slot_b(row, tube)
        for d in (2, 3, 1):
            ab_copy(v, own, d - 1, peer_z(d)).start()
        ab_copy(v, own, 3, peer_x).start()
        ab_copy(v, own, 4, peer_core).start()

    def ab_relay_z(v, d):
        slot = slot_b(row, shift(d))
        ab_copy(v, slot, 0, peer_x).wait_recv()
        ab_copy(v, slot, 4 + d, peer_x).start()
        ab_copy(v, slot, 7 + d, peer_core).start()

    def ab_relay_x(v, d):
        slot = slot_b(xrow, shift(d))
        ab_copy(v, slot, 0, peer_x).wait_recv()
        ab_copy(v, slot, 11 + d, peer_core).start()

    def ab_core(v):
        for r in (crow, lax.rem(crow + 2, 4)):
            for d in range(4):
                ab_copy(v, slot_b(r, shift(d)), 0, peer_x).wait_recv()

    def ab_finish(v):
        for n in range(15):
            ab_copy(v, 0, n, peer_x).wait_send()

    def aa_copy(buf, s_sem, r_sem, s, slot, send, device):
        return remote(buf.at[s, slot], buf.at[s, slot], s_sem.at[s, send], r_sem.at[s, slot], device)

    def aa_start(buf, s_sem, r_sem, s):
        own = col * 4 + tube
        for d in (2, 3, 1):
            aa_copy(buf, s_sem, r_sem, s, own, d - 1, peer_z(d)).start()
        aa_copy(buf, s_sem, r_sem, s, own, 3, peer_y).start()

    def aa_relay(buf, s_sem, r_sem, s):
        for d in (1, 3, 2):
            slot = col * 4 + shift(d)
            aa_copy(buf, s_sem, r_sem, s, slot, 0, peer_y).wait_recv()
            aa_copy(buf, s_sem, r_sem, s, slot, 3 + d, peer_y).start()

    def aa_rest(buf, s_sem, r_sem, s):
        for d in range(4):
            aa_copy(buf, s_sem, r_sem, s, (1 - col) * 4 + shift(d), 0, peer_y).wait_recv()
        for n in range(7):
            aa_copy(buf, s_sem, r_sem, s, 0, n, peer_y).wait_send()

    def solve_matrix(left, right):
        rows = lax.broadcasted_iota(jnp.int32, (RANK, RANK), 0)
        lanes = lax.broadcasted_iota(jnp.int32, (RANK, RANK), 1)
        return left * right + jnp.where(rows == lanes, lam, 0.0)

    def factor(left, right):
        linv[...] = inv_chol(solve_matrix(left, right), work, hinv, hlow)

    def half(q):
        return pl.ds(pl.multiple_of(q * 128, 128), 128)

    def g_swap(g, dest):
        gfin[g, half(core)] = gown[half(core)] + gpeer[g]
        cp = remote(gfin.at[g, half(core)], gfin.at[g, half(core)], s_g.at[g, 2], r_g.at[g, 2], peer_core)
        cp.start()
        remote(gfin.at[g, half(1 - core)], gfin.at[g, half(1 - core)], s_g.at[g, 2], r_g.at[g, 2], peer_core).wait_recv()
        cp.wait_send()
        dest[...] = gfin[g]

    def g_link(g, device):
        return remote(gown.at[half(core)], gpeer.at[g], s_g.at[g, 1], r_g.at[g, 1], device)

    def gram_b_start(v, g):
        gown[half(core)] = jnp.zeros((128, RANK), F32)

        def step(n, carry):
            gown[half(core)] += dot16(ball[v, n, :, half(core)], ball[v, n], 0, 0)
            return carry

        lax.fori_loop(0, 16, step, 0)
        g_link(g, peer_y).start()

    def g_link_wait(g, device):
        g_link(g, device).wait()

    def form_u(v):
        def step(n, carry):
            rows = pl.ds(pl.multiple_of(n * 256, 256), 256)
            u_buf[rows] = dot16(xh[rows], ball[v].reshape(4096, RANK), 1, 0)
            return carry

        lax.fori_loop(0, 8, step, 0)

    def tile(n):
        slot = lax.rem(n, STAGES)
        return pltpu.make_async_copy(x_ref.at[pl.ds(pl.multiple_of(n * ROWS_T, ROWS_T), ROWS_T)], xin.at[slot], load_sem.at[slot])

    n_tiles = 2048 // ROWS_T

    def convert(first, last):
        def step(n, carry):
            tile(n).wait()
            xh[pl.ds(pl.multiple_of(n * ROWS_T, ROWS_T), ROWS_T)] = xin[lax.rem(n, STAGES)].astype(BF16)
            if last < n_tiles:
                tile(n + STAGES).start()
            return carry

        lax.fori_loop(first, last, step, 0)

    ball[0, slot_b(row, tube)] = b_ref[...].astype(BF16)
    for n in range(STAGES):
        tile(n).start()
    c_cur[...] = c_ref[...]
    ab_start(0)
    part = (n_tiles - STAGES) // 4
    convert(0, part)
    ab_relay_z(0, 1)
    convert(part, 2 * part)
    ab_relay_x(0, 0)
    ab_relay_z(0, 3)
    convert(2 * part, 3 * part)
    ab_relay_z(0, 2)
    ab_relay_x(0, 1)
    convert(3 * part, 4 * part)
    convert(4 * part, n_tiles)
    ab_relay_x(0, 3)
    ab_relay_x(0, 2)
    ab_core(0)
    gram_b_start(0, 0)
    form_u(0)
    g_link_wait(0, peer_y)
    g_swap(0, gmat_b)
    ab_finish(0)

    def sweep(s, carry):
        c16 = c_cur[...].astype(BF16)
        gram_c = dot16(c16, c16, 0, 0)
        c_blk = c_cur[0:4]
        for t in range(1, 4):
            c_blk = jnp.where(tube == t, c_cur[4 * t:4 * t + 4], c_blk)

        def ya_copy(t):
            return remote(pa.at[(1 - col) * 4 + t], ya.at[s, t], s_ya.at[s, t], r_ya.at[s, t], peer_y)

        def za_copy(d):
            return remote(pa.at[col * 4 + shift(d)], za.at[s, d - 1], s_za.at[s, d - 1], r_za.at[s, d - 1], peer_z(d))

        def form_pa(slot):
            acc = None
            for k in range(4):
                term = u_buf[pl.ds(pl.multiple_of(k * 512 + slot * 64, 64), 64)] * c_blk[k:k + 1]
                acc = term if acc is None else acc + term
            pa[slot] = acc

        for d in (2, 3, 1, 0):
            form_pa((1 - col) * 4 + shift(d))
            ya_copy(shift(d)).start()
        for d in (2, 3, 1, 0):
            form_pa(col * 4 + shift(d))
        factor(gmat_b[...], gram_c)
        for d in (2, 3, 1):
            ya_copy(shift(d)).wait_recv()
            slot = col * 4 + shift(d)
            pa[slot] = pa[slot] + ya[s, shift(d)]
            za_copy(d).start()
        ya_copy(tube).wait_recv()
        total = pa[col * 4 + tube] + ya[s, tube]
        for d in (1, 3, 2):
            za_copy(d).wait_recv()
            total = total + za[s, d - 1]
        a_own = dot32(dot32(total, linv[...], 1, 1), linv[...], 1, 0)
        own_a = col * 4 + tube
        a32[s, own_a] = a_own
        a16[s, own_a] = a_own.astype(BF16)
        aa_start(a16, s_a16, r_a16, s)
        aa_start(a32, s_a32, r_a32, s)
        for k in range(4):
            csplat[k] = jnp.broadcast_to(c_blk[k:k + 1], (128, RANK)).T
        for t in range(4):
            ya_copy(t).wait_send()
        for d in range(1, 4):
            za_copy(d).wait_send()
        aa_relay(a16, s_a16, r_a16, s)
        aa_rest(a16, s_a16, r_a16, s)
        a_rows = a16[s].reshape(512, RANK)
        at_buf[...] = a_rows.astype(F32).T.astype(BF16)
        gown[...] = dot16(a_rows, a_rows, 0, 0)
        g = 1 + 2 * s
        core_gram = remote(gown.at[half(1 - core)], gcore.at[s], s_g.at[g, 0], r_g.at[g, 0], peer_core)
        core_gram.start()

        def form_pb(slot):
            acc0 = acc1 = None
            for k in range(4):
                xk = xh[k * 512:(k + 1) * 512, pl.ds(pl.multiple_of(slot * 256, 256), 256)]
                val = dot16(at_buf[...], xk, 1, 0)
                left = val[:, :128] * csplat[k]
                right = val[:, 128:] * csplat[k]
                acc0 = left if k == 0 else acc0 + left
                acc1 = right if k == 0 else acc1 + right
            pb[slot] = jnp.concatenate([acc0, acc1], axis=1)

        def order(n):
            return shift((2, 3, 1, 0)[n % 4])

        def chunk(n, q):
            xside = 1 - xpos if n < 4 else xpos
            return slot_b(xside * 2 + q, order(n))

        def yb_copy(n):
            return remote(pb.at[chunk(n, 1 - core)], yb.at[s, n], s_yb.at[s, n], r_yb.at[s, n], peer_core)

        def xb_copy(n):
            return remote(pb.at[chunk(n, core)], xb.at[s, n], s_xb.at[s, n], r_xb.at[s, n], peer_x)

        def zb_copy(d):
            return remote(pb.at[slot_b(row, shift(d))], zb.at[s, d - 1], s_zb.at[s, d - 1], r_zb.at[s, d - 1], peer_z(d))

        def merge_core(n):
            yb_copy(n).wait_recv()
            slot = chunk(n, core)
            pb[slot] = pb[slot] + yb[s, n]
            if n < 4:
                xb_copy(n).start()

        for n in range(8):
            form_pb(chunk(n, 1 - core))
            yb_copy(n).start()
            form_pb(chunk(n, core))
            if n == 0:
                core_gram.wait()
                gown[half(core)] = gown[half(core)] + gcore[s]
                g_link(g, peer_x).start()
            if n >= 1:
                merge_core(n - 1)
        merge_core(7)
        aa_relay(a32, s_a32, r_a32, s)
        g_link_wait(g, peer_x)
        g_swap(g, gmat_a)
        factor(gmat_a[...], gram_c)
        for n in range(3):
            xb_copy(n).wait_recv()
            slot = slot_b(row, order(n))
            pb[slot] = pb[slot] + xb[s, n]
            zb_copy((2, 3, 1)[n]).start()
        aa_rest(a32, s_a32, r_a32, s)
        xb_copy(3).wait_recv()
        total = pb[slot_b(row, tube)] + xb[s, 3]
        for d in (1, 3, 2):
            zb_copy(d).wait_recv()
            total = total + zb[s, d - 1]
        b_own = dot32(dot32(linv[...], total, 1, 0), linv[...], 0, 0)
        b_out[...] = b_own
        v = s + 1
        ball[v, slot_b(row, tube)] = b_own.astype(BF16)
        ab_start(v)
        for n in range(8):
            yb_copy(n).wait_send()
        for n in range(4):
            xb_copy(n).wait_send()
        for d in range(1, 4):
            zb_copy(d).wait_send()
        ab_relay_z(v, 1)
        ab_relay_z(v, 3)
        ab_relay_x(v, 0)
        ab_relay_z(v, 2)
        for d in (1, 3, 2):
            ab_relay_x(v, d)
        ab_core(v)
        gram_b_start(v, g + 1)
        form_u(v)

        cpart[s, 0] = jnp.zeros((8, RANK), F32)
        for k in range(4):
            prod = u_buf[k * 512:(k + 1) * 512] * a32[s].reshape(512, RANK)
            cpart[s, 0, k:k + 1] = jnp.sum(prod, axis=0, keepdims=True)

        def cp_copy(n):
            return remote(cpart.at[s, 0], cpart.at[s, n], s_c.at[s, n], r_c.at[s, n], plane(n))

        def ct_copy(d):
            return remote(ctot.at[s, tube], ctot.at[s, tube], s_c.at[s, 7 + d], r_c.at[s, 7 + d], peer_z(d))

        for n in range(1, 8):
            cp_copy(n).start()
        g_link_wait(g + 1, peer_y)
        g_swap(g + 1, gmat_b)
        for n in range(1, 8):
            cp_copy(n).wait_recv()
        me = col * 4 + row
        total = None
        for n in range(8):
            term = cpart[s, lax.rem(me + 8 - n, 8)]
            total = term if total is None else total + term
        ctot[s, tube] = total
        for d in range(1, 4):
            ct_copy(d).start()
        factor(gmat_a[...], gmat_b[...])
        for d in range(1, 4):
            ct_copy(d).wait_recv()
        cmid[...] = jnp.concatenate([ctot[s, t, :4] for t in range(4)], axis=0)
        c_new = dot32(dot32(cmid[...], linv[...], 1, 1), linv[...], 1, 0)
        c_cur[...] = c_new
        for n in range(1, 8):
            cp_copy(n).wait_send()
        for d in range(1, 4):
            ct_copy(d).wait_send()
        ab_finish(v)
        return carry

    lax.fori_loop(0, SWEEPS, sweep, 0)
    a_out[...] = a32[SWEEPS - 1, col * 4 + tube]
    c_out[...] = c_cur[...]


def solution(mesh):
    dma = pltpu.SemaphoreType.DMA

    def local(x_blk, b_own, c_full, ridge_lam):
        vmem = pl.BlockSpec(memory_space=pltpu.VMEM)
        return pl.pallas_call(
            kernel,
            out_shape=(
                jax.ShapeDtypeStruct((64, RANK), F32),
                jax.ShapeDtypeStruct((256, RANK), F32),
                jax.ShapeDtypeStruct((16, RANK), F32),
            ),
            in_specs=[pl.BlockSpec(memory_space=pl.ANY), vmem, vmem, vmem],
            out_specs=(vmem, vmem, vmem),
            scratch_shapes=[
                pltpu.VMEM((2048, 4096), BF16),
                pltpu.VMEM((STAGES, ROWS_T, 4096), F32),
                pltpu.VMEM((2048, RANK), F32),
                pltpu.VMEM((8, 64, RANK), F32),
                pltpu.VMEM((16, 256, 256), F32),
                pltpu.VMEM((3, 16, 256, RANK), BF16),
                pltpu.VMEM((2, 8, 64, RANK), BF16),
                pltpu.VMEM((2, 8, 64, RANK), F32),
                pltpu.VMEM((2, 4, 64, RANK), F32),
                pltpu.VMEM((2, 3, 64, RANK), F32),
                pltpu.VMEM((2, 8, 256, 256), F32),
                pltpu.VMEM((2, 4, 256, 256), F32),
                pltpu.VMEM((2, 3, 256, 256), F32),
                pltpu.VMEM((RANK, RANK), F32),
                pltpu.VMEM((2, 128, RANK), F32),
                pltpu.VMEM((5, 128, RANK), F32),
                pltpu.VMEM((5, RANK, RANK), F32),
                pltpu.VMEM((16, RANK), F32),
                pltpu.VMEM((2, 8, 8, RANK), F32),
                pltpu.VMEM((2, 4, 8, RANK), F32),
                pltpu.VMEM((4, RANK, 128), F32),
                pltpu.VMEM((RANK, 512), BF16),
                pltpu.VMEM((128, 128), F32),
                pltpu.VMEM((2, 128, 128), F32),
                pltpu.VMEM((2, 128, 128), F32),
                pltpu.VMEM((RANK, RANK), F32),
                pltpu.VMEM((RANK, RANK), F32),
                pltpu.VMEM((RANK, RANK), F32),
                pltpu.VMEM((16, RANK), F32),
                dma((STAGES,)),
                dma((3, 15)), dma((3, 16)),
                dma((2, 7)), dma((2, 8)), dma((2, 7)), dma((2, 8)),
                dma((2, 4)), dma((2, 4)), dma((2, 3)), dma((2, 3)),
                dma((2, 8)), dma((2, 8)), dma((2, 4)), dma((2, 4)), dma((2, 3)), dma((2, 3)),
                dma((5, 3)), dma((5, 3)),
                dma((2, 11)), dma((2, 11)),
            ],
            compiler_params=pltpu.CompilerParams(collective_id=0, has_side_effects=True, vmem_limit_bytes=62 * 1024 * 1024),
        )(x_blk.reshape(2048, 4096), b_own, c_full, jnp.broadcast_to(ridge_lam, (1, RANK)))

    return jax.shard_map(
        local,
        mesh=mesh,
        in_specs=(P("tube", "row", "col"), P(("col", "row", "tube"), None), P(None, None), P()),
        out_specs=(P(("row", "col", "tube"), None), P(("col", "row", "tube"), None), P(None, None)),
        check_vma=False,
    )
```

```python
import jax
import jax.numpy as jnp
from jax import lax
from jax.experimental import pallas as pl
from jax.experimental.pallas import tpu as pltpu
from jax.sharding import PartitionSpec as P

SWEEPS = 2
F32 = jnp.float32
BF16 = jnp.bfloat16
HI = lax.Precision.HIGHEST
MESH = pl.DeviceIdType.MESH
RANK = 256
PIV = 16
ROWS_T = 64
STAGES = 8


def dot32(lhs, rhs, lhs_dim, rhs_dim):
    return lax.dot_general(lhs, rhs, (((lhs_dim,), (rhs_dim,)), ((), ())), precision=HI, preferred_element_type=F32)


def dot16(lhs, rhs, lhs_dim, rhs_dim):
    return lax.dot_general(lhs, rhs, (((lhs_dim,), (rhs_dim,)), ((), ())), preferred_element_type=F32)


def factor_block(blk, w_ref, inv_ref, idx):
    size = 128
    lane = lax.broadcasted_iota(jnp.int32, (PIV, size), 1)
    row = lax.broadcasted_iota(jnp.int32, (PIV, size), 0)
    lanes = lax.broadcasted_iota(jnp.int32, (size, size), 1)
    lo = pl.multiple_of(blk * PIV, PIV)
    slab = w_ref[pl.ds(lo, PIV)]
    full = w_ref[...]
    cols = jnp.stack([jnp.broadcast_to(slab[:, q:q + 1], (PIV, size)) for q in range(PIV)])
    work = pltpu.roll(jnp.where(lane < PIV, jnp.where(lane == row, 1.0, 0.0), slab), size - PIV, 1)
    rest = pltpu.roll(jnp.where(lanes < PIV, 0.0, full), size - PIV, 1)
    scale = jnp.ones((PIV, size), F32)
    low = work
    for q in range(PIV):
        here = row == q
        piv = cols[0, q:q + 1]
        rec = 1.0 / piv
        mult = jnp.where(here, 0.0, cols[0]) * rec
        low = jnp.where(here, work * lax.rsqrt(piv), low)
        scale = jnp.where(here, rec, scale)
        work = work - mult * work[q:q + 1]
        if q + 1 < PIV:
            cols = cols[1:] - mult[None] * cols[1:, q:q + 1]
    mid = work * scale
    for q in range(PIV):
        rest = rest - full[:, q:q + 1] * mid[q:q + 1]
    w_ref[...] = rest
    low = jnp.where(lane >= size - PIV - lo, low, 0.0)
    inv_ref[idx, pl.ds(lo, PIV)] = pltpu.roll(low, lo + PIV, 1)


def inv_chol(mat, w_ref, inv_ref, low_ref, between):
    w_ref[...] = mat[:128, :128]
    lax.fori_loop(0, 128 // PIV, lambda blk, c: (factor_block(blk, w_ref, inv_ref, 0), c)[1], 0)
    low = dot32(mat[128:, :128], inv_ref[0], 1, 1)
    low_ref[...] = low
    w_ref[...] = mat[128:, 128:] - dot32(low, low, 1, 1)
    between()
    lax.fori_loop(0, 128 // PIV, lambda blk, c: (factor_block(blk, w_ref, inv_ref, 1), c)[1], 0)
    first, second = inv_ref[0], inv_ref[1]
    off = -dot32(second, dot32(low_ref[...], first, 1, 0), 1, 0)
    top = jnp.concatenate([first, jnp.zeros((128, 128), F32)], axis=1)
    return jnp.concatenate([top, jnp.concatenate([off, second], axis=1)], axis=0)


def kernel(x_ref, b_ref, c_ref, lam_ref, a_out, b_out, c_out,
           xh, xin, u_buf, pa, pb, ball, a16, a32, ya, za, yb, xb, zb,
           gown, gcore, gpeer, gfin, cmid, cpart, ctot, csplat, at_buf, work, hinv, hlow, gpart, linv, gmat_a, gmat_b, c_cur,
           load_sem, s_ab, r_ab, s_a16, r_a16, s_a32, r_a32, s_ya, r_ya, s_za, r_za,
           s_yb, r_yb, s_xb, r_xb, s_zb, r_zb, s_g, r_g, s_c, r_c):
    tube = lax.axis_index("tube")
    col = lax.axis_index("col")
    row = lax.axis_index("row")
    core = lax.rem(row, 2)
    xpos = row // 2
    xrow = lax.rem(row + 2, 4)
    crow = row + 1 - 2 * core
    lam = lam_ref[...]

    def dev(t, c, r):
        return {"tube": t, "col": c, "row": r}

    def shift(d):
        return lax.rem(tube + d, 4)

    peer_x, peer_core, peer_y = dev(tube, col, xrow), dev(tube, col, crow), dev(tube, 1 - col, row)

    pair = tube + 1 - 2 * lax.rem(tube, 2)
    mate = lax.rem(tube + 2, 4)
    near, far = 2 - tube // 2, 3 - 3 * (tube // 2)
    by_reach = (pair, near, far)
    by_need = (lax.rem(pair + 2, 4), mate, pair, tube)

    def peer_z(d):
        return dev(shift(d), col, row)

    def at_z(t):
        return dev(t, col, row)

    def plane(n):
        other = lax.rem(col * 4 + row + n, 8)
        return dev(tube, other // 4, lax.rem(other, 4))

    def tile(n):
        slot = lax.rem(n, STAGES)
        return pltpu.make_async_copy(x_ref.at[pl.ds(pl.multiple_of(n * ROWS_T, ROWS_T), ROWS_T)], xin.at[slot], load_sem.at[slot])

    n_tiles = 2048 // ROWS_T

    for n in range(STAGES):
        tile(n).start()
    barrier = pltpu.get_barrier_semaphore()
    for d in range(1, 4):
        pl.semaphore_signal(barrier, inc=1, device_id=peer_z(d), device_id_type=MESH)
    for n in range(1, 8):
        pl.semaphore_signal(barrier, inc=1, device_id=plane(n), device_id_type=MESH)
    pl.semaphore_wait(barrier, 10)

    def remote(src, dst, send, recv, device):
        return pltpu.make_async_remote_copy(src_ref=src, dst_ref=dst, send_sem=send, recv_sem=recv,
                                            device_id=device, device_id_type=MESH)

    def slot_b(r, t):
        return r * 4 + t

    def ab_copy(v, slot, send, device):
        return remote(ball.at[v, slot], ball.at[v, slot], s_ab.at[v, send], r_ab.at[v, slot], device)

    def ab_start(v):
        own = slot_b(row, tube)
        ab_copy(v, own, 3, peer_x).start()
        ab_copy(v, own, 4, peer_core).start()
        for n in range(3):
            ab_copy(v, own, n, at_z(by_reach[n])).start()

    def ab_relay_z(v, n):
        slot = slot_b(row, by_reach[n])
        ab_copy(v, slot, 0, peer_x).wait_recv()
        ab_copy(v, slot, 5 + n, peer_x).start()
        ab_copy(v, slot, 8 + n, peer_core).start()
        return slot

    def ab_relay_x(v, n):
        slot = slot_b(xrow, tube if n == 3 else by_reach[n])
        ab_copy(v, slot, 0, peer_x).wait_recv()
        ab_copy(v, slot, 11 + n, peer_core).start()
        return slot

    def ab_core(v, r, n):
        slot = slot_b(r, tube if n == 3 else by_reach[n])
        ab_copy(v, slot, 0, peer_x).wait_recv()
        return slot

    def ab_finish(v):
        for n in range(15):
            ab_copy(v, 0, n, peer_x).wait_send()

    def aa_copy(buf, s_sem, r_sem, s, slot, send, device):
        return remote(buf.at[s, slot], buf.at[s, slot], s_sem.at[s, send], r_sem.at[s, slot], device)

    def aa_start(buf, s_sem, r_sem, s):
        own = col * 4 + tube
        aa_copy(buf, s_sem, r_sem, s, own, 3, peer_y).start()
        for n in range(3):
            aa_copy(buf, s_sem, r_sem, s, own, n, at_z(by_reach[n])).start()

    def aa_relay(buf, s_sem, r_sem, s):
        for n in range(3):
            slot = col * 4 + by_reach[n]
            aa_copy(buf, s_sem, r_sem, s, slot, 0, peer_y).wait_recv()
            aa_copy(buf, s_sem, r_sem, s, slot, 4 + n, peer_y).start()

    def aa_rest(buf, s_sem, r_sem, s):
        for d in range(4):
            aa_copy(buf, s_sem, r_sem, s, (1 - col) * 4 + shift(d), 0, peer_y).wait_recv()
        for n in range(7):
            aa_copy(buf, s_sem, r_sem, s, 0, n, peer_y).wait_send()

    def solve_matrix(left, right):
        rows = lax.broadcasted_iota(jnp.int32, (RANK, RANK), 0)
        lanes = lax.broadcasted_iota(jnp.int32, (RANK, RANK), 1)
        return left * right + jnp.where(rows == lanes, lam, 0.0)

    def factor(left, right, between=lambda: None):
        linv[...] = inv_chol(solve_matrix(left, right), work, hinv, hlow, between)

    def half(q):
        return pl.ds(pl.multiple_of(q * 128, 128), 128)

    def g_swap(g, dest):
        gfin[g, half(core)] = gown[half(core)] + gpeer[g]
        cp = remote(gfin.at[g, half(core)], gfin.at[g, half(core)], s_g.at[g, 2], r_g.at[g, 2], peer_core)
        cp.start()
        remote(gfin.at[g, half(1 - core)], gfin.at[g, half(1 - core)], s_g.at[g, 2], r_g.at[g, 2], peer_core).wait_recv()
        cp.wait_send()
        dest[...] = gfin[g]

    def g_link(g, device):
        return remote(gown.at[half(core)], gpeer.at[g], s_g.at[g, 1], r_g.at[g, 1], device)

    def g_link_wait(g, device):
        g_link(g, device).wait()

    def take_group(v, slots, first=False):
        def step(n, carry):
            rows = pl.ds(pl.multiple_of(n * 512, 512), 512)
            total = None if first else u_buf[rows]
            for slot in slots:
                term = dot16(xh[rows, pl.ds(pl.multiple_of(slot * 256, 256), 256)], ball[v, slot], 1, 0)
                total = term if total is None else total + term
            u_buf[rows] = total
            return carry

        lax.fori_loop(0, 4, step, 0)
        for slot in slots:
            gpart[slot] = dot16(ball[v, slot, :, half(core)], ball[v, slot], 0, 0)

    def gram_b_sum(g):
        total = gpart[0]
        for n in range(1, 16):
            total = total + gpart[n]
        gown[half(core)] = total
        g_link(g, peer_y).start()

    def convert(first, last):
        def step(n, carry):
            tile(n).wait()
            xh[pl.ds(pl.multiple_of(n * ROWS_T, ROWS_T), ROWS_T)] = xin[lax.rem(n, STAGES)].astype(BF16)
            if last < n_tiles:
                tile(n + STAGES).start()
            return carry

        lax.fori_loop(first, last, step, 0)

    ball[0, slot_b(row, tube)] = b_ref[...].astype(BF16)
    c_cur[...] = c_ref[...]
    ab_start(0)
    part = (n_tiles - STAGES) // 4
    across = lax.rem(crow + 2, 4)
    convert(0, part)
    ab_relay_z(0, 0)
    ab_relay_x(0, 3)
    convert(part, 3 * part)
    ab_relay_x(0, 0)
    convert(3 * part, 4 * part)
    convert(4 * part, n_tiles)
    take_group(0, (slot_b(row, tube), slot_b(row, pair), slot_b(xrow, tube), ab_core(0, crow, 3)), True)
    take_group(0, (slot_b(xrow, pair), ab_relay_z(0, 1), ab_core(0, crow, 0), ab_core(0, across, 3)))
    take_group(0, (ab_relay_z(0, 2), ab_relay_x(0, 1), ab_core(0, crow, 1), ab_core(0, across, 0)))
    take_group(0, (ab_relay_x(0, 2), ab_core(0, crow, 2), ab_core(0, across, 1), ab_core(0, across, 2)))
    gram_b_sum(0)
    g_link_wait(0, peer_y)
    g_swap(0, gmat_b)
    ab_finish(0)

    def sweep(s, carry):
        c16 = c_cur[...].astype(BF16)
        gram_c = dot16(c16, c16, 0, 0)
        c_blk = c_cur[0:4]
        for t in range(1, 4):
            c_blk = jnp.where(tube == t, c_cur[4 * t:4 * t + 4], c_blk)

        def ya_copy(t):
            return remote(pa.at[(1 - col) * 4 + t], ya.at[s, t], s_ya.at[s, t], r_ya.at[s, t], peer_y)

        def za_copy(n):
            return remote(pa.at[col * 4 + by_need[n]], za.at[s, n], s_za.at[s, n], r_za.at[s, n], at_z(mate if n == 1 else pair))

        def merge_a(n):
            ya_copy(by_need[n]).wait_recv()
            slot = col * 4 + by_need[n]
            both = pa[slot] + ya[s, by_need[n]]
            if n == 1:
                za_copy(0).wait_recv()
                both = both + za[s, 0]
            pa[slot] = both
            za_copy(n).start()

        def form_pa(slot):
            acc = None
            for k in range(4):
                term = u_buf[pl.ds(pl.multiple_of(k * 512 + slot * 64, 64), 64)] * c_blk[k:k + 1]
                acc = term if acc is None else acc + term
            pa[slot] = acc

        for n in range(4):
            form_pa((1 - col) * 4 + by_need[n])
            ya_copy(by_need[n]).start()
        for n in range(4):
            form_pa(col * 4 + by_need[n])
        merge_a(0)

        def middle_a():
            merge_a(1)
            merge_a(2)

        factor(gmat_b[...], gram_c, middle_a)
        ya_copy(tube).wait_recv()
        total = pa[col * 4 + tube] + ya[s, tube]
        for n in (2, 1):
            za_copy(n).wait_recv()
            total = total + za[s, n]
        a_own = dot32(dot32(total, linv[...], 1, 1), linv[...], 1, 0)
        own_a = col * 4 + tube
        a32[s, own_a] = a_own
        a16[s, own_a] = a_own.astype(BF16)
        aa_start(a16, s_a16, r_a16, s)
        for k in range(4):
            csplat[k] = jnp.broadcast_to(c_blk[k:k + 1], (128, RANK)).T
        for t in range(4):
            ya_copy(t).wait_send()
        for n in range(3):
            za_copy(n).wait_send()
        aa_relay(a16, s_a16, r_a16, s)
        aa_rest(a16, s_a16, r_a16, s)
        a_rows = a16[s].reshape(512, RANK)
        at_buf[...] = a_rows.astype(F32).T.astype(BF16)
        gown[...] = dot16(a_rows, a_rows, 0, 0)
        g = 1 + 2 * s
        core_gram = remote(gown.at[half(1 - core)], gcore.at[s], s_g.at[g, 0], r_g.at[g, 0], peer_core)
        core_gram.start()
        aa_start(a32, s_a32, r_a32, s)

        def form_pb(slot):
            acc0 = acc1 = None
            for k in range(4):
                xk = xh[k * 512:(k + 1) * 512, pl.ds(pl.multiple_of(slot * 256, 256), 256)]
                val = dot16(at_buf[...], xk, 1, 0)
                left = val[:, :128] * csplat[k]
                right = val[:, 128:] * csplat[k]
                acc0 = left if k == 0 else acc0 + left
                acc1 = right if k == 0 else acc1 + right
            pb[slot] = jnp.concatenate([acc0, acc1], axis=1)

        def order(n):
            return by_need[n % 4]

        def chunk(n, q):
            xside = 1 - xpos if n < 4 else xpos
            return slot_b(xside * 2 + q, order(n))

        def yb_copy(n):
            return remote(pb.at[chunk(n, 1 - core)], yb.at[s, n], s_yb.at[s, n], r_yb.at[s, n], peer_core)

        def xb_copy(n):
            return remote(pb.at[chunk(n, core)], xb.at[s, n], s_xb.at[s, n], r_xb.at[s, n], peer_x)

        def zb_copy(n):
            return remote(pb.at[slot_b(row, by_need[n])], zb.at[s, n], s_zb.at[s, n], r_zb.at[s, n], at_z(mate if n == 1 else pair))

        def merge_b(n):
            xb_copy(n).wait_recv()
            slot = slot_b(row, by_need[n])
            both = pb[slot] + xb[s, n]
            if n == 1:
                zb_copy(0).wait_recv()
                both = both + zb[s, 0]
            pb[slot] = both
            zb_copy(n).start()

        def merge_core(n):
            yb_copy(n).wait_recv()
            slot = chunk(n, core)
            pb[slot] = pb[slot] + yb[s, n]
            if n < 4:
                xb_copy(n).start()

        for n in range(8):
            form_pb(chunk(n, 1 - core))
            yb_copy(n).start()
            form_pb(chunk(n, core))
            if n == 2:
                core_gram.wait()
                gown[half(core)] = gown[half(core)] + gcore[s]
                g_link(g, peer_x).start()
            if n >= 1:
                merge_core(n - 1)
        merge_core(7)
        merge_b(0)
        aa_relay(a32, s_a32, r_a32, s)
        g_link_wait(g, peer_x)
        g_swap(g, gmat_a)
        merge_b(1)
        factor(gmat_a[...], gram_c)
        merge_b(2)
        aa_rest(a32, s_a32, r_a32, s)
        xb_copy(3).wait_recv()
        total = pb[slot_b(row, tube)] + xb[s, 3]
        for n in (2, 1):
            zb_copy(n).wait_recv()
            total = total + zb[s, n]
        b_own = dot32(dot32(linv[...], total, 1, 0), linv[...], 0, 0)
        b_out[...] = b_own
        v = s + 1
        ball[v, slot_b(row, tube)] = b_own.astype(BF16)
        ab_start(v)
        for n in range(8):
            yb_copy(n).wait_send()
        for n in range(4):
            xb_copy(n).wait_send()
        for n in range(3):
            zb_copy(n).wait_send()
        take_group(v, (slot_b(row, tube), ab_relay_z(v, 0), ab_relay_x(v, 3), ab_core(v, crow, 3)), True)
        take_group(v, (ab_relay_x(v, 0), ab_relay_z(v, 1), ab_core(v, crow, 0), ab_core(v, across, 3)))
        take_group(v, (ab_relay_z(v, 2), ab_relay_x(v, 1), ab_core(v, crow, 1), ab_core(v, across, 0)))
        take_group(v, (ab_relay_x(v, 2), ab_core(v, crow, 2), ab_core(v, across, 1), ab_core(v, across, 2)))
        gram_b_sum(g + 1)

        cpart[s, 0] = jnp.zeros((8, RANK), F32)
        for k in range(4):
            prod = u_buf[k * 512:(k + 1) * 512] * a32[s].reshape(512, RANK)
            cpart[s, 0, k:k + 1] = jnp.sum(prod, axis=0, keepdims=True)

        def cp_copy(n):
            return remote(cpart.at[s, 0], cpart.at[s, n], s_c.at[s, n], r_c.at[s, n], plane(n))

        def ct_copy(d):
            return remote(ctot.at[s, tube], ctot.at[s, tube], s_c.at[s, 7 + d], r_c.at[s, 7 + d], peer_z(d))

        for n in range(1, 8):
            cp_copy(n).start()
        g_link_wait(g + 1, peer_y)
        g_swap(g + 1, gmat_b)
        for n in range(1, 8):
            cp_copy(n).wait_recv()
        me = col * 4 + row
        total = None
        for n in range(8):
            term = cpart[s, lax.rem(me + 8 - n, 8)]
            total = term if total is None else total + term
        ctot[s, tube] = total
        for d in range(1, 4):
            ct_copy(d).start()
        factor(gmat_a[...], gmat_b[...])
        for d in range(1, 4):
            ct_copy(d).wait_recv()
        cmid[...] = jnp.concatenate([ctot[s, t, :4] for t in range(4)], axis=0)
        c_new = dot32(dot32(cmid[...], linv[...], 1, 1), linv[...], 1, 0)
        c_cur[...] = c_new
        for n in range(1, 8):
            cp_copy(n).wait_send()
        for d in range(1, 4):
            ct_copy(d).wait_send()
        ab_finish(v)
        return carry

    lax.fori_loop(0, SWEEPS, sweep, 0)
    a_out[...] = a32[SWEEPS - 1, col * 4 + tube]
    c_out[...] = c_cur[...]


def solution(mesh):
    dma = pltpu.SemaphoreType.DMA

    def local(x_blk, b_own, c_full, ridge_lam):
        vmem = pl.BlockSpec(memory_space=pltpu.VMEM)
        return pl.pallas_call(
            kernel,
            out_shape=(
                jax.ShapeDtypeStruct((64, RANK), F32),
                jax.ShapeDtypeStruct((256, RANK), F32),
                jax.ShapeDtypeStruct((16, RANK), F32),
            ),
            in_specs=[pl.BlockSpec(memory_space=pl.ANY), vmem, vmem, vmem],
            out_specs=(vmem, vmem, vmem),
            scratch_shapes=[
                pltpu.VMEM((2048, 4096), BF16),
                pltpu.VMEM((STAGES, ROWS_T, 4096), F32),
                pltpu.VMEM((2048, RANK), F32),
                pltpu.VMEM((8, 64, RANK), F32),
                pltpu.VMEM((16, 256, 256), F32),
                pltpu.VMEM((3, 16, 256, RANK), BF16),
                pltpu.VMEM((2, 8, 64, RANK), BF16),
                pltpu.VMEM((2, 8, 64, RANK), F32),
                pltpu.VMEM((2, 4, 64, RANK), F32),
                pltpu.VMEM((2, 3, 64, RANK), F32),
                pltpu.VMEM((2, 8, 256, 256), F32),
                pltpu.VMEM((2, 4, 256, 256), F32),
                pltpu.VMEM((2, 3, 256, 256), F32),
                pltpu.VMEM((RANK, RANK), F32),
                pltpu.VMEM((2, 128, RANK), F32),
                pltpu.VMEM((5, 128, RANK), F32),
                pltpu.VMEM((5, RANK, RANK), F32),
                pltpu.VMEM((16, RANK), F32),
                pltpu.VMEM((2, 8, 8, RANK), F32),
                pltpu.VMEM((2, 4, 8, RANK), F32),
                pltpu.VMEM((4, RANK, 128), F32),
                pltpu.VMEM((RANK, 512), BF16),
                pltpu.VMEM((128, 128), F32),
                pltpu.VMEM((2, 128, 128), F32),
                pltpu.VMEM((128, 128), F32),
                pltpu.VMEM((16, 128, RANK), F32),
                pltpu.VMEM((RANK, RANK), F32),
                pltpu.VMEM((RANK, RANK), F32),
                pltpu.VMEM((RANK, RANK), F32),
                pltpu.VMEM((16, RANK), F32),
                dma((STAGES,)),
                dma((3, 15)), dma((3, 16)),
                dma((2, 7)), dma((2, 8)), dma((2, 7)), dma((2, 8)),
                dma((2, 4)), dma((2, 4)), dma((2, 3)), dma((2, 3)),
                dma((2, 8)), dma((2, 8)), dma((2, 4)), dma((2, 4)), dma((2, 3)), dma((2, 3)),
                dma((5, 3)), dma((5, 3)),
                dma((2, 11)), dma((2, 11)),
            ],
            compiler_params=pltpu.CompilerParams(collective_id=0, has_side_effects=True, vmem_limit_bytes=62 * 1024 * 1024),
        )(x_blk.reshape(2048, 4096), b_own, c_full, jnp.broadcast_to(ridge_lam, (1, RANK)))

    return jax.shard_map(
        local,
        mesh=mesh,
        in_specs=(P("tube", "row", "col"), P(("col", "row", "tube"), None), P(None, None), P()),
        out_specs=(P(("row", "col", "tube"), None), P(("col", "row", "tube"), None), P(None, None)),
        check_vma=False,
    )
```

```python
import jax
import jax.numpy as jnp
from jax import lax
from jax.experimental import pallas as pl
from jax.experimental.pallas import tpu as pltpu
from jax.sharding import PartitionSpec as P

SWEEPS = 2
F32 = jnp.float32
BF16 = jnp.bfloat16
HI = lax.Precision.HIGHEST
MESH = pl.DeviceIdType.MESH
RANK = 256
PIV = 16
ROWS_T = 64
STAGES = 8


def dot32(lhs, rhs, lhs_dim, rhs_dim):
    return lax.dot_general(lhs, rhs, (((lhs_dim,), (rhs_dim,)), ((), ())), precision=HI, preferred_element_type=F32)


def dot16(lhs, rhs, lhs_dim, rhs_dim):
    return lax.dot_general(lhs, rhs, (((lhs_dim,), (rhs_dim,)), ((), ())), preferred_element_type=F32)


def factor_block(blk, w_ref, inv_ref, idx, top):
    size = 128
    lane = lax.broadcasted_iota(jnp.int32, (PIV, size), 1)
    row = lax.broadcasted_iota(jnp.int32, (PIV, size), 0)
    lanes = lax.broadcasted_iota(jnp.int32, (size - top, size), 1)
    lo = pl.multiple_of(blk * PIV, PIV)
    slab = w_ref[pl.ds(lo, PIV)]
    full = w_ref[top:]
    cols = jnp.stack([jnp.broadcast_to(slab[:, q:q + 1], (PIV, size)) for q in range(PIV)])
    work = pltpu.roll(jnp.where(lane < PIV, jnp.where(lane == row, 1.0, 0.0), slab), size - PIV, 1)
    rest = pltpu.roll(jnp.where(lanes < PIV, 0.0, full), size - PIV, 1)
    scale = jnp.ones((PIV, size), F32)
    low = work
    for q in range(PIV):
        here = row == q
        piv = cols[0, q:q + 1]
        rec = 1.0 / piv
        mult = jnp.where(here, 0.0, cols[0]) * rec
        low = jnp.where(here, work * lax.rsqrt(piv), low)
        scale = jnp.where(here, rec, scale)
        work = work - mult * work[q:q + 1]
        if q + 1 < PIV:
            cols = cols[1:] - mult[None] * cols[1:, q:q + 1]
    mid = work * scale
    for q in range(PIV):
        rest = rest - full[:, q:q + 1] * mid[q:q + 1]
    w_ref[top:] = rest
    low = jnp.where(lane >= size - PIV - lo, low, 0.0)
    inv_ref[idx, pl.ds(lo, PIV)] = pltpu.roll(low, lo + PIV, 1)


def factor_half(w_ref, inv_ref, idx):
    for first, last in ((0, 4), (4, 8)):
        lax.fori_loop(first, last, lambda blk, c: (factor_block(blk, w_ref, inv_ref, idx, first * PIV), c)[1], 0)


def inv_chol(mat, w_ref, inv_ref, low_ref, between):
    w_ref[...] = mat[:128, :128]
    factor_half(w_ref, inv_ref, 0)
    low = dot32(mat[128:, :128], inv_ref[0], 1, 1)
    low_ref[...] = low
    w_ref[...] = mat[128:, 128:] - dot32(low, low, 1, 1)
    between()
    factor_half(w_ref, inv_ref, 1)
    first, second = inv_ref[0], inv_ref[1]
    off = -dot32(second, dot32(low_ref[...], first, 1, 0), 1, 0)
    top = jnp.concatenate([first, jnp.zeros((128, 128), F32)], axis=1)
    return jnp.concatenate([top, jnp.concatenate([off, second], axis=1)], axis=0)


def kernel(x_ref, b_ref, c_ref, lam_ref, a_out, b_out, c_out,
           xh, xin, u_buf, pa, pb, ball, a16, a32, ya, za, yb, xb, zb,
           gown, gcore, gpeer, gfin, cmid, cpart, ctot, csplat, at_buf, work, hinv, hlow, gpart, linv, gmat_a, gmat_b, c_cur,
           load_sem, s_ab, r_ab, s_a16, r_a16, s_a32, r_a32, s_ya, r_ya, s_za, r_za,
           s_yb, r_yb, s_xb, r_xb, s_zb, r_zb, s_g, r_g, s_c, r_c):
    tube = lax.axis_index("tube")
    col = lax.axis_index("col")
    row = lax.axis_index("row")
    core = lax.rem(row, 2)
    xpos = row // 2
    xrow = lax.rem(row + 2, 4)
    crow = row + 1 - 2 * core
    lam = lam_ref[...]

    def dev(t, c, r):
        return {"tube": t, "col": c, "row": r}

    def shift(d):
        return lax.rem(tube + d, 4)

    peer_x, peer_core, peer_y = dev(tube, col, xrow), dev(tube, col, crow), dev(tube, 1 - col, row)

    pair = tube + 1 - 2 * lax.rem(tube, 2)
    mate = lax.rem(tube + 2, 4)
    near, far = 2 - tube // 2, 3 - 3 * (tube // 2)
    by_reach = (pair, near, far)
    by_need = (lax.rem(pair + 2, 4), mate, pair, tube)

    def peer_z(d):
        return dev(shift(d), col, row)

    def at_z(t):
        return dev(t, col, row)

    def plane(n):
        other = lax.rem(col * 4 + row + n, 8)
        return dev(tube, other // 4, lax.rem(other, 4))

    def tile(n):
        slot = lax.rem(n, STAGES)
        return pltpu.make_async_copy(x_ref.at[pl.ds(pl.multiple_of(n * ROWS_T, ROWS_T), ROWS_T)], xin.at[slot], load_sem.at[slot])

    n_tiles = 2048 // ROWS_T

    for n in range(STAGES):
        tile(n).start()
    barrier = pltpu.get_barrier_semaphore()
    for d in range(1, 4):
        pl.semaphore_signal(barrier, inc=1, device_id=peer_z(d), device_id_type=MESH)
    for n in range(1, 8):
        pl.semaphore_signal(barrier, inc=1, device_id=plane(n), device_id_type=MESH)
    pl.semaphore_wait(barrier, 10)

    def remote(src, dst, send, recv, device):
        return pltpu.make_async_remote_copy(src_ref=src, dst_ref=dst, send_sem=send, recv_sem=recv,
                                            device_id=device, device_id_type=MESH)

    def slot_b(r, t):
        return r * 4 + t

    def ab_copy(v, slot, send, device):
        return remote(ball.at[v, slot], ball.at[v, slot], s_ab.at[v, send], r_ab.at[v, slot], device)

    def ab_start(v):
        own = slot_b(row, tube)
        ab_copy(v, own, 3, peer_x).start()
        ab_copy(v, own, 4, peer_core).start()
        for n in range(3):
            ab_copy(v, own, n, at_z(by_reach[n])).start()

    def ab_relay_z(v, n):
        slot = slot_b(row, by_reach[n])
        ab_copy(v, slot, 0, peer_x).wait_recv()
        ab_copy(v, slot, 5 + n, peer_x).start()
        ab_copy(v, slot, 8 + n, peer_core).start()
        return slot

    def ab_relay_x(v, n):
        slot = slot_b(xrow, tube if n == 3 else by_reach[n])
        ab_copy(v, slot, 0, peer_x).wait_recv()
        ab_copy(v, slot, 11 + n, peer_core).start()
        return slot

    def ab_core(v, r, n):
        slot = slot_b(r, tube if n == 3 else by_reach[n])
        ab_copy(v, slot, 0, peer_x).wait_recv()
        return slot

    def ab_finish(v):
        for n in range(15):
            ab_copy(v, 0, n, peer_x).wait_send()

    def aa_copy(buf, s_sem, r_sem, s, slot, send, device):
        return remote(buf.at[s, slot], buf.at[s, slot], s_sem.at[s, send], r_sem.at[s, slot], device)

    def aa_start(buf, s_sem, r_sem, s):
        own = col * 4 + tube
        aa_copy(buf, s_sem, r_sem, s, own, 3, peer_y).start()
        for n in range(3):
            aa_copy(buf, s_sem, r_sem, s, own, n, at_z(by_reach[n])).start()

    def aa_relay(buf, s_sem, r_sem, s):
        for n in range(3):
            slot = col * 4 + by_reach[n]
            aa_copy(buf, s_sem, r_sem, s, slot, 0, peer_y).wait_recv()
            aa_copy(buf, s_sem, r_sem, s, slot, 4 + n, peer_y).start()

    def aa_rest(buf, s_sem, r_sem, s):
        for d in range(4):
            aa_copy(buf, s_sem, r_sem, s, (1 - col) * 4 + shift(d), 0, peer_y).wait_recv()
        for n in range(7):
            aa_copy(buf, s_sem, r_sem, s, 0, n, peer_y).wait_send()

    def solve_matrix(left, right):
        rows = lax.broadcasted_iota(jnp.int32, (RANK, RANK), 0)
        lanes = lax.broadcasted_iota(jnp.int32, (RANK, RANK), 1)
        return left * right + jnp.where(rows == lanes, lam, 0.0)

    def factor(left, right, between=lambda: None):
        linv[...] = inv_chol(solve_matrix(left, right), work, hinv, hlow, between)

    def half(q):
        return pl.ds(pl.multiple_of(q * 128, 128), 128)

    def g_swap(g, dest):
        gfin[g, half(core)] = gown[half(core)] + gpeer[g]
        cp = remote(gfin.at[g, half(core)], gfin.at[g, half(core)], s_g.at[g, 2], r_g.at[g, 2], peer_core)
        cp.start()
        remote(gfin.at[g, half(1 - core)], gfin.at[g, half(1 - core)], s_g.at[g, 2], r_g.at[g, 2], peer_core).wait_recv()
        cp.wait_send()
        dest[...] = gfin[g]

    def g_link(g, device):
        return remote(gown.at[half(core)], gpeer.at[g], s_g.at[g, 1], r_g.at[g, 1], device)

    def g_link_wait(g, device):
        g_link(g, device).wait()

    def take_group(v, slots, first=False, after=lambda: None):
        for slot in slots:
            gpart[slot] = dot16(ball[v, slot, :, half(core)], ball[v, slot], 0, 0)
        after()

        def step(n, carry):
            rows = pl.ds(pl.multiple_of(n * 512, 512), 512)
            total = None if first else u_buf[rows]
            for slot in slots:
                term = dot16(xh[rows, pl.ds(pl.multiple_of(slot * 256, 256), 256)], ball[v, slot], 1, 0)
                total = term if total is None else total + term
            u_buf[rows] = total
            return carry

        lax.fori_loop(0, 4, step, 0)

    def gram_b_sum(g):
        total = gpart[0]
        for n in range(1, 16):
            total = total + gpart[n]
        gown[half(core)] = total
        g_link(g, peer_y).start()

    def convert(first, last):
        def step(n, carry):
            tile(n).wait()
            xh[pl.ds(pl.multiple_of(n * ROWS_T, ROWS_T), ROWS_T)] = xin[lax.rem(n, STAGES)].astype(BF16)
            if last < n_tiles:
                tile(n + STAGES).start()
            return carry

        lax.fori_loop(first, last, step, 0)

    ball[0, slot_b(row, tube)] = b_ref[...].astype(BF16)
    c_cur[...] = c_ref[...]
    ab_start(0)
    part = (n_tiles - STAGES) // 4
    across = lax.rem(crow + 2, 4)
    convert(0, part)
    ab_relay_z(0, 0)
    ab_relay_x(0, 3)
    convert(part, 3 * part)
    ab_relay_x(0, 0)
    convert(3 * part, 4 * part)
    convert(4 * part, n_tiles)
    take_group(0, (slot_b(row, tube), slot_b(row, pair), slot_b(xrow, tube), ab_core(0, crow, 3)), True)
    take_group(0, (slot_b(xrow, pair), ab_relay_z(0, 1), ab_core(0, crow, 0), ab_core(0, across, 3)))
    take_group(0, (ab_relay_z(0, 2), ab_relay_x(0, 1), ab_core(0, crow, 1), ab_core(0, across, 0)))
    take_group(0, (ab_relay_x(0, 2), ab_core(0, crow, 2), ab_core(0, across, 1), ab_core(0, across, 2)),
               after=lambda: gram_b_sum(0))
    g_link_wait(0, peer_y)
    g_swap(0, gmat_b)
    ab_finish(0)

    def sweep(s, carry):
        c16 = c_cur[...].astype(BF16)
        gram_c = dot16(c16, c16, 0, 0)
        c_blk = c_cur[0:4]
        for t in range(1, 4):
            c_blk = jnp.where(tube == t, c_cur[4 * t:4 * t + 4], c_blk)

        def ya_copy(t):
            return remote(pa.at[(1 - col) * 4 + t], ya.at[s, t], s_ya.at[s, t], r_ya.at[s, t], peer_y)

        def za_copy(n):
            return remote(pa.at[col * 4 + by_need[n]], za.at[s, n], s_za.at[s, n], r_za.at[s, n], at_z(mate if n == 1 else pair))

        def merge_a(n):
            ya_copy(by_need[n]).wait_recv()
            slot = col * 4 + by_need[n]
            both = pa[slot] + ya[s, by_need[n]]
            if n == 1:
                za_copy(0).wait_recv()
                both = both + za[s, 0]
            pa[slot] = both
            za_copy(n).start()

        def form_pa(slot):
            acc = None
            for k in range(4):
                term = u_buf[pl.ds(pl.multiple_of(k * 512 + slot * 64, 64), 64)] * c_blk[k:k + 1]
                acc = term if acc is None else acc + term
            pa[slot] = acc

        for n in range(4):
            form_pa((1 - col) * 4 + by_need[n])
            ya_copy(by_need[n]).start()
        for n in range(4):
            form_pa(col * 4 + by_need[n])
        merge_a(0)

        def middle_a():
            merge_a(1)
            merge_a(2)

        factor(gmat_b[...], gram_c, middle_a)
        ya_copy(tube).wait_recv()
        total = pa[col * 4 + tube] + ya[s, tube]
        for n in (2, 1):
            za_copy(n).wait_recv()
            total = total + za[s, n]
        a_own = dot32(dot32(total, linv[...], 1, 1), linv[...], 1, 0)
        own_a = col * 4 + tube
        a32[s, own_a] = a_own
        a16[s, own_a] = a_own.astype(BF16)
        aa_start(a16, s_a16, r_a16, s)
        for k in range(4):
            csplat[k] = jnp.broadcast_to(c_blk[k:k + 1], (128, RANK)).T
        for t in range(4):
            ya_copy(t).wait_send()
        for n in range(3):
            za_copy(n).wait_send()
        aa_relay(a16, s_a16, r_a16, s)
        aa_rest(a16, s_a16, r_a16, s)
        a_rows = a16[s].reshape(512, RANK)
        at_buf[...] = a_rows.astype(F32).T.astype(BF16)
        gown[...] = dot16(a_rows, a_rows, 0, 0)
        g = 1 + 2 * s
        core_gram = remote(gown.at[half(1 - core)], gcore.at[s], s_g.at[g, 0], r_g.at[g, 0], peer_core)
        core_gram.start()
        aa_start(a32, s_a32, r_a32, s)

        def form_pb(slot):
            acc0 = acc1 = None
            for k in range(4):
                xk = xh[k * 512:(k + 1) * 512, pl.ds(pl.multiple_of(slot * 256, 256), 256)]
                val = dot16(at_buf[...], xk, 1, 0)
                left = val[:, :128] * csplat[k]
                right = val[:, 128:] * csplat[k]
                acc0 = left if k == 0 else acc0 + left
                acc1 = right if k == 0 else acc1 + right
            pb[slot] = jnp.concatenate([acc0, acc1], axis=1)

        def order(n):
            return by_need[n % 4]

        def chunk(n, q):
            xside = 1 - xpos if n < 4 else xpos
            return slot_b(xside * 2 + q, order(n))

        def yb_copy(n):
            return remote(pb.at[chunk(n, 1 - core)], yb.at[s, n], s_yb.at[s, n], r_yb.at[s, n], peer_core)

        def xb_copy(n):
            return remote(pb.at[chunk(n, core)], xb.at[s, n], s_xb.at[s, n], r_xb.at[s, n], peer_x)

        def zb_copy(n):
            return remote(pb.at[slot_b(row, by_need[n])], zb.at[s, n], s_zb.at[s, n], r_zb.at[s, n], at_z(mate if n == 1 else pair))

        def merge_b(n):
            xb_copy(n).wait_recv()
            slot = slot_b(row, by_need[n])
            both = pb[slot] + xb[s, n]
            if n == 1:
                zb_copy(0).wait_recv()
                both = both + zb[s, 0]
            pb[slot] = both
            zb_copy(n).start()

        def merge_core(n):
            yb_copy(n).wait_recv()
            slot = chunk(n, core)
            pb[slot] = pb[slot] + yb[s, n]
            if n < 4:
                xb_copy(n).start()

        for n in range(8):
            form_pb(chunk(n, 1 - core))
            yb_copy(n).start()
            form_pb(chunk(n, core))
            if n == 2:
                core_gram.wait()
                gown[half(core)] = gown[half(core)] + gcore[s]
                g_link(g, peer_x).start()
            if n >= 1:
                merge_core(n - 1)
        merge_core(7)
        merge_b(0)
        aa_relay(a32, s_a32, r_a32, s)
        g_link_wait(g, peer_x)
        g_swap(g, gmat_a)
        merge_b(1)
        factor(gmat_a[...], gram_c)
        merge_b(2)
        aa_rest(a32, s_a32, r_a32, s)
        xb_copy(3).wait_recv()
        total = pb[slot_b(row, tube)] + xb[s, 3]
        for n in (2, 1):
            zb_copy(n).wait_recv()
            total = total + zb[s, n]
        b_own = dot32(dot32(linv[...], total, 1, 0), linv[...], 0, 0)
        b_out[...] = b_own
        v = s + 1
        ball[v, slot_b(row, tube)] = b_own.astype(BF16)
        ab_start(v)
        for n in range(8):
            yb_copy(n).wait_send()
        for n in range(4):
            xb_copy(n).wait_send()
        for n in range(3):
            zb_copy(n).wait_send()
        take_group(v, (slot_b(row, tube), ab_relay_z(v, 0), ab_relay_x(v, 3), ab_core(v, crow, 3)), True)
        take_group(v, (ab_relay_x(v, 0), ab_relay_z(v, 1), ab_core(v, crow, 0), ab_core(v, across, 3)))
        take_group(v, (ab_relay_z(v, 2), ab_relay_x(v, 1), ab_core(v, crow, 1), ab_core(v, across, 0)))
        take_group(v, (ab_core(v, crow, 2), ab_core(v, across, 1)))
        take_group(v, (ab_relay_x(v, 2), ab_core(v, across, 2)),
                   after=lambda: gram_b_sum(g + 1))

        cpart[s, 0] = jnp.zeros((8, RANK), F32)
        for k in range(4):
            prod = u_buf[k * 512:(k + 1) * 512] * a32[s].reshape(512, RANK)
            cpart[s, 0, k:k + 1] = jnp.sum(prod, axis=0, keepdims=True)

        def cp_copy(n):
            return remote(cpart.at[s, 0], cpart.at[s, n], s_c.at[s, n], r_c.at[s, n], plane(n))

        def ct_copy(d):
            return remote(ctot.at[s, tube], ctot.at[s, tube], s_c.at[s, 7 + d], r_c.at[s, 7 + d], peer_z(d))

        for n in range(1, 8):
            cp_copy(n).start()
        g_link_wait(g + 1, peer_y)
        g_swap(g + 1, gmat_b)
        for n in range(1, 8):
            cp_copy(n).wait_recv()
        me = col * 4 + row
        total = None
        for n in range(8):
            term = cpart[s, lax.rem(me + 8 - n, 8)]
            total = term if total is None else total + term
        ctot[s, tube] = total
        for d in range(1, 4):
            ct_copy(d).start()
        factor(gmat_a[...], gmat_b[...])
        for d in range(1, 4):
            ct_copy(d).wait_recv()
        cmid[...] = jnp.concatenate([ctot[s, t, :4] for t in range(4)], axis=0)
        c_new = dot32(dot32(cmid[...], linv[...], 1, 1), linv[...], 1, 0)
        c_cur[...] = c_new
        for n in range(1, 8):
            cp_copy(n).wait_send()
        for d in range(1, 4):
            ct_copy(d).wait_send()
        ab_finish(v)
        return carry

    lax.fori_loop(0, SWEEPS, sweep, 0)
    a_out[...] = a32[SWEEPS - 1, col * 4 + tube]
    c_out[...] = c_cur[...]


def solution(mesh):
    dma = pltpu.SemaphoreType.DMA

    def local(x_blk, b_own, c_full, ridge_lam):
        vmem = pl.BlockSpec(memory_space=pltpu.VMEM)
        return pl.pallas_call(
            kernel,
            out_shape=(
                jax.ShapeDtypeStruct((64, RANK), F32),
                jax.ShapeDtypeStruct((256, RANK), F32),
                jax.ShapeDtypeStruct((16, RANK), F32),
            ),
            in_specs=[pl.BlockSpec(memory_space=pl.ANY), vmem, vmem, vmem],
            out_specs=(vmem, vmem, vmem),
            scratch_shapes=[
                pltpu.VMEM((2048, 4096), BF16),
                pltpu.VMEM((STAGES, ROWS_T, 4096), F32),
                pltpu.VMEM((2048, RANK), F32),
                pltpu.VMEM((8, 64, RANK), F32),
                pltpu.VMEM((16, 256, 256), F32),
                pltpu.VMEM((3, 16, 256, RANK), BF16),
                pltpu.VMEM((2, 8, 64, RANK), BF16),
                pltpu.VMEM((2, 8, 64, RANK), F32),
                pltpu.VMEM((2, 4, 64, RANK), F32),
                pltpu.VMEM((2, 3, 64, RANK), F32),
                pltpu.VMEM((2, 8, 256, 256), F32),
                pltpu.VMEM((2, 4, 256, 256), F32),
                pltpu.VMEM((2, 3, 256, 256), F32),
                pltpu.VMEM((RANK, RANK), F32),
                pltpu.VMEM((2, 128, RANK), F32),
                pltpu.VMEM((5, 128, RANK), F32),
                pltpu.VMEM((5, RANK, RANK), F32),
                pltpu.VMEM((16, RANK), F32),
                pltpu.VMEM((2, 8, 8, RANK), F32),
                pltpu.VMEM((2, 4, 8, RANK), F32),
                pltpu.VMEM((4, RANK, 128), F32),
                pltpu.VMEM((RANK, 512), BF16),
                pltpu.VMEM((128, 128), F32),
                pltpu.VMEM((2, 128, 128), F32),
                pltpu.VMEM((128, 128), F32),
                pltpu.VMEM((16, 128, RANK), F32),
                pltpu.VMEM((RANK, RANK), F32),
                pltpu.VMEM((RANK, RANK), F32),
                pltpu.VMEM((RANK, RANK), F32),
                pltpu.VMEM((16, RANK), F32),
                dma((STAGES,)),
                dma((3, 15)), dma((3, 16)),
                dma((2, 7)), dma((2, 8)), dma((2, 7)), dma((2, 8)),
                dma((2, 4)), dma((2, 4)), dma((2, 3)), dma((2, 3)),
                dma((2, 8)), dma((2, 8)), dma((2, 4)), dma((2, 4)), dma((2, 3)), dma((2, 3)),
                dma((5, 3)), dma((5, 3)),
                dma((2, 11)), dma((2, 11)),
            ],
            compiler_params=pltpu.CompilerParams(collective_id=0, has_side_effects=True, vmem_limit_bytes=62 * 1024 * 1024),
        )(x_blk.reshape(2048, 4096), b_own, c_full, jnp.broadcast_to(ridge_lam, (1, RANK)))

    return jax.shard_map(
        local,
        mesh=mesh,
        in_specs=(P("tube", "row", "col"), P(("col", "row", "tube"), None), P(None, None), P()),
        out_specs=(P(("row", "col", "tube"), None), P(("col", "row", "tube"), None), P(None, None)),
        check_vma=False,
    )
```

```python
import jax
import jax.numpy as jnp
from jax import lax
from jax.experimental import pallas as pl
from jax.experimental.pallas import tpu as pltpu
from jax.sharding import PartitionSpec as P

SWEEPS = 2
F32 = jnp.float32
BF16 = jnp.bfloat16
HI = lax.Precision.HIGHEST
MESH = pl.DeviceIdType.MESH
RANK = 256
PIV = 16
ROWS_T = 64
STAGES = 8


def dot32(lhs, rhs, lhs_dim, rhs_dim):
    return lax.dot_general(lhs, rhs, (((lhs_dim,), (rhs_dim,)), ((), ())), precision=HI, preferred_element_type=F32)


def dot16(lhs, rhs, lhs_dim, rhs_dim):
    return lax.dot_general(lhs, rhs, (((lhs_dim,), (rhs_dim,)), ((), ())), preferred_element_type=F32)


def factor_block(blk, w_ref, inv_ref, idx, top):
    size = 128
    lane = lax.broadcasted_iota(jnp.int32, (PIV, size), 1)
    row = lax.broadcasted_iota(jnp.int32, (PIV, size), 0)
    lanes = lax.broadcasted_iota(jnp.int32, (size - top, size), 1)
    lo = pl.multiple_of(blk * PIV, PIV)
    slab = w_ref[pl.ds(lo, PIV)]
    full = w_ref[top:]
    cols = jnp.stack([jnp.broadcast_to(slab[:, q:q + 1], (PIV, size)) for q in range(PIV)])
    work = pltpu.roll(jnp.where(lane < PIV, jnp.where(lane == row, 1.0, 0.0), slab), size - PIV, 1)
    rest = pltpu.roll(jnp.where(lanes < PIV, 0.0, full), size - PIV, 1)
    scale = jnp.ones((PIV, size), F32)
    low = work
    for q in range(PIV):
        here = row == q
        piv = cols[0, q:q + 1]
        rec = 1.0 / piv
        mult = jnp.where(here, 0.0, cols[0]) * rec
        low = jnp.where(here, work * lax.rsqrt(piv), low)
        scale = jnp.where(here, rec, scale)
        work = work - mult * work[q:q + 1]
        if q + 1 < PIV:
            cols = cols[1:] - mult[None] * cols[1:, q:q + 1]
    mid = work * scale
    for q in range(PIV):
        rest = rest - full[:, q:q + 1] * mid[q:q + 1]
    w_ref[top:] = rest
    low = jnp.where(lane >= size - PIV - lo, low, 0.0)
    inv_ref[idx, pl.ds(lo, PIV)] = pltpu.roll(low, lo + PIV, 1)


def factor_half(w_ref, inv_ref, idx):
    for first, last in ((0, 2), (2, 4), (4, 6), (6, 8)):
        lax.fori_loop(first, last, lambda blk, c: (factor_block(blk, w_ref, inv_ref, idx, first * PIV), c)[1], 0)


def inv_chol(mat, w_ref, inv_ref, low_ref, between):
    w_ref[...] = mat[:128, :128]
    factor_half(w_ref, inv_ref, 0)
    low = dot32(mat[128:, :128], inv_ref[0], 1, 1)
    low_ref[...] = low
    w_ref[...] = mat[128:, 128:] - dot32(low, low, 1, 1)
    between()
    factor_half(w_ref, inv_ref, 1)
    first, second = inv_ref[0], inv_ref[1]
    off = -dot32(second, dot32(low_ref[...], first, 1, 0), 1, 0)
    top = jnp.concatenate([first, jnp.zeros((128, 128), F32)], axis=1)
    return jnp.concatenate([top, jnp.concatenate([off, second], axis=1)], axis=0)


def kernel(x_ref, b_ref, c_ref, lam_ref, a_out, b_out, c_out,
           xh, xin, u_buf, pa, pb, ball, a16, a32, ya, za, yb, xb, zb,
           gown, gcore, gpeer, gfin, cmid, cpart, ctot, csplat, at_buf, work, hinv, hlow, gpart, linv, gmat_a, gmat_b, c_cur,
           load_sem, s_ab, r_ab, s_a16, r_a16, s_a32, r_a32, s_ya, r_ya, s_za, r_za,
           s_yb, r_yb, s_xb, r_xb, s_zb, r_zb, s_g, r_g, s_c, r_c):
    tube = lax.axis_index("tube")
    col = lax.axis_index("col")
    row = lax.axis_index("row")
    core = lax.rem(row, 2)
    xpos = row // 2
    xrow = lax.rem(row + 2, 4)
    crow = row + 1 - 2 * core
    lam = lam_ref[...]

    def dev(t, c, r):
        return {"tube": t, "col": c, "row": r}

    def shift(d):
        return lax.rem(tube + d, 4)

    peer_x, peer_core, peer_y = dev(tube, col, xrow), dev(tube, col, crow), dev(tube, 1 - col, row)

    pair = tube + 1 - 2 * lax.rem(tube, 2)
    mate = lax.rem(tube + 2, 4)
    near, far = 2 - tube // 2, 3 - 3 * (tube // 2)
    by_reach = (pair, near, far)
    by_need = (lax.rem(pair + 2, 4), mate, pair, tube)

    def peer_z(d):
        return dev(shift(d), col, row)

    def at_z(t):
        return dev(t, col, row)

    def plane(n):
        other = lax.rem(col * 4 + row + n, 8)
        return dev(tube, other // 4, lax.rem(other, 4))

    def tile(n):
        slot = lax.rem(n, STAGES)
        return pltpu.make_async_copy(x_ref.at[pl.ds(pl.multiple_of(n * ROWS_T, ROWS_T), ROWS_T)], xin.at[slot], load_sem.at[slot])

    n_tiles = 2048 // ROWS_T

    for n in range(STAGES):
        tile(n).start()
    barrier = pltpu.get_barrier_semaphore()
    for d in range(1, 4):
        pl.semaphore_signal(barrier, inc=1, device_id=peer_z(d), device_id_type=MESH)
    for n in range(1, 8):
        pl.semaphore_signal(barrier, inc=1, device_id=plane(n), device_id_type=MESH)
    pl.semaphore_wait(barrier, 10)

    def remote(src, dst, send, recv, device):
        return pltpu.make_async_remote_copy(src_ref=src, dst_ref=dst, send_sem=send, recv_sem=recv,
                                            device_id=device, device_id_type=MESH)

    def slot_b(r, t):
        return r * 4 + t

    def ab_copy(v, slot, send, device):
        return remote(ball.at[v, slot], ball.at[v, slot], s_ab.at[v, send], r_ab.at[v, slot], device)

    def ab_start(v):
        own = slot_b(row, tube)
        ab_copy(v, own, 3, peer_x).start()
        ab_copy(v, own, 4, peer_core).start()
        for n in range(3):
            ab_copy(v, own, n, at_z(by_reach[n])).start()

    def ab_relay_z(v, n):
        slot = slot_b(row, by_reach[n])
        ab_copy(v, slot, 0, peer_x).wait_recv()
        ab_copy(v, slot, 5 + n, peer_x).start()
        ab_copy(v, slot, 8 + n, peer_core).start()
        return slot

    def ab_relay_x(v, n):
        slot = slot_b(xrow, tube if n == 3 else by_reach[n])
        ab_copy(v, slot, 0, peer_x).wait_recv()
        ab_copy(v, slot, 11 + n, peer_core).start()
        return slot

    def ab_core(v, r, n):
        slot = slot_b(r, tube if n == 3 else by_reach[n])
        ab_copy(v, slot, 0, peer_x).wait_recv()
        return slot

    def ab_finish(v):
        for n in range(15):
            ab_copy(v, 0, n, peer_x).wait_send()

    def aa_copy(buf, s_sem, r_sem, s, slot, send, device):
        return remote(buf.at[s, slot], buf.at[s, slot], s_sem.at[s, send], r_sem.at[s, slot], device)

    def aa_start(buf, s_sem, r_sem, s):
        own = col * 4 + tube
        aa_copy(buf, s_sem, r_sem, s, own, 3, peer_y).start()
        for n in range(3):
            aa_copy(buf, s_sem, r_sem, s, own, n, at_z(by_reach[n])).start()

    def aa_relay(buf, s_sem, r_sem, s):
        for n in range(3):
            slot = col * 4 + by_reach[n]
            aa_copy(buf, s_sem, r_sem, s, slot, 0, peer_y).wait_recv()
            aa_copy(buf, s_sem, r_sem, s, slot, 4 + n, peer_y).start()

    def aa_rest(buf, s_sem, r_sem, s):
        for d in range(4):
            aa_copy(buf, s_sem, r_sem, s, (1 - col) * 4 + shift(d), 0, peer_y).wait_recv()
        for n in range(7):
            aa_copy(buf, s_sem, r_sem, s, 0, n, peer_y).wait_send()

    def solve_matrix(left, right):
        rows = lax.broadcasted_iota(jnp.int32, (RANK, RANK), 0)
        lanes = lax.broadcasted_iota(jnp.int32, (RANK, RANK), 1)
        return left * right + jnp.where(rows == lanes, lam, 0.0)

    def factor(left, right, between=lambda: None):
        linv[...] = inv_chol(solve_matrix(left, right), work, hinv, hlow, between)

    def half(q):
        return pl.ds(pl.multiple_of(q * 128, 128), 128)

    def g_swap(g, dest):
        gfin[g, half(core)] = gown[half(core)] + gpeer[g]
        cp = remote(gfin.at[g, half(core)], gfin.at[g, half(core)], s_g.at[g, 2], r_g.at[g, 2], peer_core)
        cp.start()
        remote(gfin.at[g, half(1 - core)], gfin.at[g, half(1 - core)], s_g.at[g, 2], r_g.at[g, 2], peer_core).wait_recv()
        cp.wait_send()
        dest[...] = gfin[g]

    def g_link(g, device):
        return remote(gown.at[half(core)], gpeer.at[g], s_g.at[g, 1], r_g.at[g, 1], device)

    def g_link_wait(g, device):
        g_link(g, device).wait()

    def take_group(v, slots, first=False, after=lambda: None):
        for slot in slots:
            gpart[slot] = dot16(ball[v, slot, :, half(core)], ball[v, slot], 0, 0)
        after()

        def step(n, carry):
            rows = pl.ds(pl.multiple_of(n * 512, 512), 512)
            total = None if first else u_buf[rows]
            for slot in slots:
                term = dot16(xh[rows, pl.ds(pl.multiple_of(slot * 256, 256), 256)], ball[v, slot], 1, 0)
                total = term if total is None else total + term
            u_buf[rows] = total
            return carry

        lax.fori_loop(0, 4, step, 0)

    def gram_b_sum(g):
        total = gpart[0]
        for n in range(1, 16):
            total = total + gpart[n]
        gown[half(core)] = total
        g_link(g, peer_y).start()

    def convert(first, last):
        def step(n, carry):
            tile(n).wait()
            xh[pl.ds(pl.multiple_of(n * ROWS_T, ROWS_T), ROWS_T)] = xin[lax.rem(n, STAGES)].astype(BF16)
            if last < n_tiles:
                tile(n + STAGES).start()
            return carry

        lax.fori_loop(first, last, step, 0)

    ball[0, slot_b(row, tube)] = b_ref[...].astype(BF16)
    c_cur[...] = c_ref[...]
    ab_start(0)
    part = (n_tiles - STAGES) // 4
    across = lax.rem(crow + 2, 4)
    convert(0, part)
    ab_relay_z(0, 0)
    ab_relay_x(0, 3)
    convert(part, 3 * part)
    ab_relay_x(0, 0)
    convert(3 * part, 4 * part)
    convert(4 * part, n_tiles)
    take_group(0, (slot_b(row, tube), slot_b(row, pair), slot_b(xrow, tube), ab_core(0, crow, 3)), True)
    take_group(0, (slot_b(xrow, pair), ab_relay_z(0, 1), ab_core(0, crow, 0), ab_core(0, across, 3)))
    take_group(0, (ab_relay_z(0, 2), ab_relay_x(0, 1), ab_core(0, crow, 1), ab_core(0, across, 0)))
    take_group(0, (ab_relay_x(0, 2), ab_core(0, crow, 2), ab_core(0, across, 1), ab_core(0, across, 2)),
               after=lambda: gram_b_sum(0))
    g_link_wait(0, peer_y)
    g_swap(0, gmat_b)
    ab_finish(0)

    def sweep(s, carry):
        c16 = c_cur[...].astype(BF16)
        gram_c = dot16(c16, c16, 0, 0)
        c_blk = c_cur[0:4]
        for t in range(1, 4):
            c_blk = jnp.where(tube == t, c_cur[4 * t:4 * t + 4], c_blk)

        def ya_copy(t):
            return remote(pa.at[(1 - col) * 4 + t], ya.at[s, t], s_ya.at[s, t], r_ya.at[s, t], peer_y)

        def za_copy(n):
            return remote(pa.at[col * 4 + by_need[n]], za.at[s, n], s_za.at[s, n], r_za.at[s, n], at_z(mate if n == 1 else pair))

        def merge_a(n):
            ya_copy(by_need[n]).wait_recv()
            slot = col * 4 + by_need[n]
            both = pa[slot] + ya[s, by_need[n]]
            if n == 1:
                za_copy(0).wait_recv()
                both = both + za[s, 0]
            pa[slot] = both
            za_copy(n).start()

        def form_pa(slot):
            acc = None
            for k in range(4):
                term = u_buf[pl.ds(pl.multiple_of(k * 512 + slot * 64, 64), 64)] * c_blk[k:k + 1]
                acc = term if acc is None else acc + term
            pa[slot] = acc

        for n in range(4):
            form_pa((1 - col) * 4 + by_need[n])
            ya_copy(by_need[n]).start()
        for n in range(4):
            form_pa(col * 4 + by_need[n])
        merge_a(0)

        def middle_a():
            merge_a(1)
            merge_a(2)

        factor(gmat_b[...], gram_c, middle_a)
        ya_copy(tube).wait_recv()
        total = pa[col * 4 + tube] + ya[s, tube]
        for n in (2, 1):
            za_copy(n).wait_recv()
            total = total + za[s, n]
        a_own = dot32(dot32(total, linv[...], 1, 1), linv[...], 1, 0)
        own_a = col * 4 + tube
        a32[s, own_a] = a_own
        a16[s, own_a] = a_own.astype(BF16)
        aa_start(a16, s_a16, r_a16, s)
        for k in range(4):
            csplat[k] = jnp.broadcast_to(c_blk[k:k + 1], (128, RANK)).T
        for t in range(4):
            ya_copy(t).wait_send()
        for n in range(3):
            za_copy(n).wait_send()
        aa_relay(a16, s_a16, r_a16, s)
        aa_rest(a16, s_a16, r_a16, s)
        a_rows = a16[s].reshape(512, RANK)
        at_buf[...] = a_rows.astype(F32).T.astype(BF16)
        gown[...] = dot16(a_rows, a_rows, 0, 0)
        g = 1 + 2 * s
        core_gram = remote(gown.at[half(1 - core)], gcore.at[s], s_g.at[g, 0], r_g.at[g, 0], peer_core)
        core_gram.start()
        aa_start(a32, s_a32, r_a32, s)

        def form_pb(slot):
            acc0 = acc1 = None
            for k in range(4):
                xk = xh[k * 512:(k + 1) * 512, pl.ds(pl.multiple_of(slot * 256, 256), 256)]
                val = dot16(at_buf[...], xk, 1, 0)
                left = val[:, :128] * csplat[k]
                right = val[:, 128:] * csplat[k]
                acc0 = left if k == 0 else acc0 + left
                acc1 = right if k == 0 else acc1 + right
            pb[slot] = jnp.concatenate([acc0, acc1], axis=1)

        def order(n):
            return by_need[n % 4]

        def chunk(n, q):
            xside = 1 - xpos if n < 4 else xpos
            return slot_b(xside * 2 + q, order(n))

        def yb_copy(n):
            return remote(pb.at[chunk(n, 1 - core)], yb.at[s, n], s_yb.at[s, n], r_yb.at[s, n], peer_core)

        def xb_copy(n):
            return remote(pb.at[chunk(n, core)], xb.at[s, n], s_xb.at[s, n], r_xb.at[s, n], peer_x)

        def zb_copy(n):
            return remote(pb.at[slot_b(row, by_need[n])], zb.at[s, n], s_zb.at[s, n], r_zb.at[s, n], at_z(mate if n == 1 else pair))

        def merge_b(n):
            xb_copy(n).wait_recv()
            slot = slot_b(row, by_need[n])
            both = pb[slot] + xb[s, n]
            if n == 1:
                zb_copy(0).wait_recv()
                both = both + zb[s, 0]
            pb[slot] = both
            zb_copy(n).start()

        def merge_core(n):
            yb_copy(n).wait_recv()
            slot = chunk(n, core)
            pb[slot] = pb[slot] + yb[s, n]
            if n < 4:
                xb_copy(n).start()

        for n in range(8):
            form_pb(chunk(n, 1 - core))
            yb_copy(n).start()
            form_pb(chunk(n, core))
            if n == 2:
                core_gram.wait()
                gown[half(core)] = gown[half(core)] + gcore[s]
                g_link(g, peer_x).start()
            if n >= 1:
                merge_core(n - 1)
        merge_core(7)
        merge_b(0)
        aa_relay(a32, s_a32, r_a32, s)
        g_link_wait(g, peer_x)
        g_swap(g, gmat_a)
        merge_b(1)
        factor(gmat_a[...], gram_c)
        merge_b(2)
        aa_rest(a32, s_a32, r_a32, s)
        xb_copy(3).wait_recv()
        total = pb[slot_b(row, tube)] + xb[s, 3]
        for n in (2, 1):
            zb_copy(n).wait_recv()
            total = total + zb[s, n]
        b_own = dot32(dot32(linv[...], total, 1, 0), linv[...], 0, 0)
        b_out[...] = b_own
        v = s + 1
        ball[v, slot_b(row, tube)] = b_own.astype(BF16)
        ab_start(v)
        for n in range(8):
            yb_copy(n).wait_send()
        for n in range(4):
            xb_copy(n).wait_send()
        for n in range(3):
            zb_copy(n).wait_send()
        take_group(v, (slot_b(row, tube), ab_relay_z(v, 0), ab_relay_x(v, 3), ab_core(v, crow, 3)), True)
        take_group(v, (ab_relay_x(v, 0), ab_relay_z(v, 1), ab_core(v, crow, 0), ab_core(v, across, 3)))
        take_group(v, (ab_relay_z(v, 2), ab_relay_x(v, 1), ab_core(v, crow, 1), ab_core(v, across, 0)))
        take_group(v, (ab_core(v, crow, 2), ab_core(v, across, 1)))
        take_group(v, (ab_relay_x(v, 2), ab_core(v, across, 2)),
                   after=lambda: gram_b_sum(g + 1))

        cpart[s, 0] = jnp.zeros((8, RANK), F32)
        for k in range(4):
            prod = u_buf[k * 512:(k + 1) * 512] * a32[s].reshape(512, RANK)
            cpart[s, 0, k:k + 1] = jnp.sum(prod, axis=0, keepdims=True)

        def cp_copy(n):
            return remote(cpart.at[s, 0], cpart.at[s, n], s_c.at[s, n], r_c.at[s, n], plane(n))

        def ct_copy(d):
            return remote(ctot.at[s, tube], ctot.at[s, tube], s_c.at[s, 7 + d], r_c.at[s, 7 + d], peer_z(d))

        for n in range(1, 8):
            cp_copy(n).start()
        g_link_wait(g + 1, peer_y)
        g_swap(g + 1, gmat_b)
        for n in range(1, 8):
            cp_copy(n).wait_recv()
        me = col * 4 + row
        total = None
        for n in range(8):
            term = cpart[s, lax.rem(me + 8 - n, 8)]
            total = term if total is None else total + term
        ctot[s, tube] = total
        for d in range(1, 4):
            ct_copy(d).start()
        factor(gmat_a[...], gmat_b[...])
        for d in range(1, 4):
            ct_copy(d).wait_recv()
        cmid[...] = jnp.concatenate([ctot[s, t, :4] for t in range(4)], axis=0)
        c_new = dot32(dot32(cmid[...], linv[...], 1, 1), linv[...], 1, 0)
        c_cur[...] = c_new
        for n in range(1, 8):
            cp_copy(n).wait_send()
        for d in range(1, 4):
            ct_copy(d).wait_send()
        ab_finish(v)
        return carry

    lax.fori_loop(0, SWEEPS, sweep, 0)
    a_out[...] = a32[SWEEPS - 1, col * 4 + tube]
    c_out[...] = c_cur[...]


def solution(mesh):
    dma = pltpu.SemaphoreType.DMA

    def local(x_blk, b_own, c_full, ridge_lam):
        vmem = pl.BlockSpec(memory_space=pltpu.VMEM)
        return pl.pallas_call(
            kernel,
            out_shape=(
                jax.ShapeDtypeStruct((64, RANK), F32),
                jax.ShapeDtypeStruct((256, RANK), F32),
                jax.ShapeDtypeStruct((16, RANK), F32),
            ),
            in_specs=[pl.BlockSpec(memory_space=pl.ANY), vmem, vmem, vmem],
            out_specs=(vmem, vmem, vmem),
            scratch_shapes=[
                pltpu.VMEM((2048, 4096), BF16),
                pltpu.VMEM((STAGES, ROWS_T, 4096), F32),
                pltpu.VMEM((2048, RANK), F32),
                pltpu.VMEM((8, 64, RANK), F32),
                pltpu.VMEM((16, 256, 256), F32),
                pltpu.VMEM((3, 16, 256, RANK), BF16),
                pltpu.VMEM((2, 8, 64, RANK), BF16),
                pltpu.VMEM((2, 8, 64, RANK), F32),
                pltpu.VMEM((2, 4, 64, RANK), F32),
                pltpu.VMEM((2, 3, 64, RANK), F32),
                pltpu.VMEM((2, 8, 256, 256), F32),
                pltpu.VMEM((2, 4, 256, 256), F32),
                pltpu.VMEM((2, 3, 256, 256), F32),
                pltpu.VMEM((RANK, RANK), F32),
                pltpu.VMEM((2, 128, RANK), F32),
                pltpu.VMEM((5, 128, RANK), F32),
                pltpu.VMEM((5, RANK, RANK), F32),
                pltpu.VMEM((16, RANK), F32),
                pltpu.VMEM((2, 8, 8, RANK), F32),
                pltpu.VMEM((2, 4, 8, RANK), F32),
                pltpu.VMEM((4, RANK, 128), F32),
                pltpu.VMEM((RANK, 512), BF16),
                pltpu.VMEM((128, 128), F32),
                pltpu.VMEM((2, 128, 128), F32),
                pltpu.VMEM((128, 128), F32),
                pltpu.VMEM((16, 128, RANK), F32),
                pltpu.VMEM((RANK, RANK), F32),
                pltpu.VMEM((RANK, RANK), F32),
                pltpu.VMEM((RANK, RANK), F32),
                pltpu.VMEM((16, RANK), F32),
                dma((STAGES,)),
                dma((3, 15)), dma((3, 16)),
                dma((2, 7)), dma((2, 8)), dma((2, 7)), dma((2, 8)),
                dma((2, 4)), dma((2, 4)), dma((2, 3)), dma((2, 3)),
                dma((2, 8)), dma((2, 8)), dma((2, 4)), dma((2, 4)), dma((2, 3)), dma((2, 3)),
                dma((5, 3)), dma((5, 3)),
                dma((2, 11)), dma((2, 11)),
            ],
            compiler_params=pltpu.CompilerParams(collective_id=0, has_side_effects=True, vmem_limit_bytes=62 * 1024 * 1024),
        )(x_blk.reshape(2048, 4096), b_own, c_full, jnp.broadcast_to(ridge_lam, (1, RANK)))

    return jax.shard_map(
        local,
        mesh=mesh,
        in_specs=(P("tube", "row", "col"), P(("col", "row", "tube"), None), P(None, None), P()),
        out_specs=(P(("row", "col", "tube"), None), P(("col", "row", "tube"), None), P(None, None)),
        check_vma=False,
    )
```
